32 devices in a mesh: dp: 4 (over z), stage: 2 (over y), tp: 4 (over x, core).
Axes of the slice: x: 2, y: 2, z: 4, core: 2. Of those that a mesh axis runs over, the one named last changes fastest.
Arguments:
- act_in: bfloat16 [2, 32, 14, 14, 1024], P('stage', ('dp', 'tp'))
- w_conv: bfloat16 [2, 3, 3, 1024, 1024], P('stage', None, None, None, 'tp')
- gamma_vec: float32 [2, 1024], P('stage', 'tp')
- beta_vec: float32 [2, 1024], P('stage', 'tp')
- z_grad: bfloat16 [2, 32, 14, 14, 1024], P('stage', 'dp', None, None, 'tp')
Outputs:
- output 1: bfloat16 [2, 32, 14, 14, 1024], P('stage', 'dp', None, None, 'tp')
- output 2: bfloat16 [2, 32, 14, 14, 1024], P('stage', ('dp', 'tp'))
- output 3: float32 [2, 3, 3, 1024, 1024], P('stage', None, None, None, 'tp')
All inputs are finite; a program needn't handle non-finite values.
Results may differ from the reference program's by a relative error of at most 0.00473.
Values are sent between devices in bfloat16 or wider.
A program may use at most 1 GiB of HBM per device.

```python
import jax
import jax.numpy as jnp
from jax import lax

STAGES = 2
IMAGES = 32
IMG_SIDE = 14
CH_IN = 1024
CH_OUT = 1024


def put_at(stage_pos, values):
    widths = [(stage_pos, STAGES - 1 - stage_pos)] + [(0, 0)] * values.ndim
    return jnp.pad(values[None], widths)


def setup_inputs(seed: int = 0) -> dict:
    base_key = jax.random.key(seed)
    k_act, k_w, k_gam, k_beta, k_dz = jax.random.split(base_key, 5)
    act_vals = jax.random.normal(k_act, (IMAGES, IMG_SIDE, IMG_SIDE, CH_IN), jnp.float32)
    w_vals = jax.random.normal(k_w, (3, 3, CH_IN, CH_OUT), jnp.float32) * (9 * CH_IN) ** -0.5
    gamma_vals = 1.0 + 0.3 * jax.random.normal(k_gam, (CH_OUT,), jnp.float32)
    beta_vals = 0.5 * jax.random.normal(k_beta, (CH_OUT,), jnp.float32)
    dz_vals = jax.random.normal(k_dz, (IMAGES, IMG_SIDE, IMG_SIDE, CH_OUT), jnp.float32)
    return {
        'act_in': put_at(0, act_vals.astype(jnp.bfloat16)),
        'w_conv': put_at(1, w_vals.astype(jnp.bfloat16)),
        'gamma_vec': put_at(1, gamma_vals),
        'beta_vec': put_at(1, beta_vals),
        'z_grad': put_at(1, dz_vals.astype(jnp.bfloat16)),
    }


def conv_same(images, kernel):
    return lax.conv_general_dilated(images, kernel, (1, 1), 'SAME', dimension_numbers=('NHWC', 'HWIO', 'NHWC'))


def reference(act_in, w_conv, gamma_vec, beta_vec, z_grad):
    kernel = w_conv[1].astype(jnp.float32)
    gamma_row = gamma_vec[1]
    beta_row = beta_vec[1]

    def one_image(w_acc, img_pair):
        image_hwc, dz_hwc = img_pair
        image_f = image_hwc[None].astype(jnp.float32)
        pre_act, pull_back = jax.vjp(conv_same, image_f, kernel)
        affine = pre_act * gamma_row + beta_row
        z_img = jnp.maximum(affine, 0.0).astype(jnp.bfloat16)
        grad_pre = jnp.where(affine > 0, dz_hwc[None].astype(jnp.float32) * gamma_row, 0.0).astype(jnp.bfloat16)
        image_grad, kernel_grad = pull_back(grad_pre.astype(jnp.float32))
        return w_acc + kernel_grad, (z_img[0], image_grad[0].astype(jnp.bfloat16))

    w_init = jnp.zeros(kernel.shape, jnp.float32)
    w_sum, (z_all, dact_all) = lax.scan(one_image, w_init, (act_in[0], z_grad[1]))
    return put_at(1, z_all), put_at(0, dact_all), put_at(1, w_sum)
```

```python
import jax
import jax.numpy as jnp
from jax import lax
from jax.sharding import PartitionSpec as P


AXES = ('dp', 'stage', 'tp')


def conv_fwd(images, kernel):
    return lax.conv_general_dilated(images, kernel, (1, 1), 'SAME', dimension_numbers=('NHWC', 'HWIO', 'NHWC'), preferred_element_type=jnp.float32)


def conv_input_grad(grad_map, kernel):
    flipped = lax.rev(kernel, (0, 1))
    return lax.conv_general_dilated(grad_map, flipped, (1, 1), 'SAME', dimension_numbers=('NHWC', 'HWOI', 'NHWC'), preferred_element_type=jnp.float32)


def conv_kernel_grad(images, grad_map):
    return lax.conv_general_dilated(images, grad_map, (1, 1), ((1, 1), (1, 1)), dimension_numbers=('CHWN', 'IHWO', 'HWNC'), preferred_element_type=jnp.float32)


def solution(mesh):
    act_spec = P('stage', ('dp', 'tp'))
    w_spec = P('stage', None, None, None, 'tp')
    vec_spec = P('stage', 'tp')
    chan_spec = P('stage', 'dp', None, None, 'tp')
    n_dp, n_tp = mesh.shape['dp'], mesh.shape['tp']

    def at(d, s, t):
        return (d * 2 + s) * n_tp + t

    every = [(d, t) for d in range(n_dp) for t in range(n_tp)]
    to_conv = [(at(d, 0, t), at(d, 1, t)) for d, t in every]
    to_home = [(at(d, 1, t), at(d, 0, t)) for d, t in every]
    ring_home = [(at(d, 0, t), at((d + 1) % n_dp, 0, t)) for d, t in every]
    ring_conv = [(at(d, 1, t), at((d + 1) % n_dp, 1, t)) for d, t in every]
    swap_core = [(at(d, 1, t), at(d, 1, t ^ 1)) for d, t in every]
    swap_chip = [(at(d, 1, t), at(d, 1, t ^ 2)) for d, t in every]

    def move(v, pairs):
        return lax.ppermute(v, AXES, perm=pairs)

    def device_step(act_in, w_conv, gamma_vec, beta_vec, z_grad):
        tp = lax.axis_index('tp')
        on_conv = lax.axis_index('stage') == 1
        kernel = w_conv[0]
        gamma_row = gamma_vec[0]
        beta_row = beta_vec[0]

        def spread(block):
            other = move(block, swap_chip)
            return block, other

        near = move(act_in[0], to_conv)
        far = move(near, swap_chip)
        near_x = jnp.concatenate([near, move(near, swap_core)])
        far_x = jnp.concatenate([far, move(far, swap_core)])

        dz = z_grad[0].reshape(4, 2, 14, 14, -1)

        def dz_of(rel):
            return lax.dynamic_index_in_dim(dz, jnp.bitwise_xor(tp, rel), 0, keepdims=False)

        def forward(images, rel):
            affine = conv_fwd(images, kernel) * gamma_row + beta_row
            z_part = jnp.maximum(affine, 0.0).astype(jnp.bfloat16)
            dz_part = jnp.concatenate([dz_of(rel), dz_of(rel + 1)])
            grad_pre = jnp.where(affine > 0, dz_part * gamma_row, 0.0).astype(jnp.bfloat16)
            return z_part, grad_pre

        z_near, g_near = forward(near_x, 0)
        z_far, g_far = forward(far_x, 2)

        xs = [jnp.concatenate([near_x, far_x])]
        gs = [jnp.concatenate([g_near, g_far])]
        home = act_in[0]
        g_n, g_f = g_near, g_far
        for _ in range(n_dp - 1):
            home = move(home, ring_home)
            a = move(home, to_conv)
            b = move(a, swap_chip)
            pair = jnp.concatenate([a, b])
            xs.append(jnp.concatenate([pair, move(pair, swap_core)]))
            g_n, g_f = move(g_n, ring_conv), move(g_f, ring_conv)
            gs.append(jnp.concatenate([g_n[:2], g_f[:2], g_n[2:], g_f[2:]]))

        part_far = conv_input_grad(g_far, kernel)
        part_near = conv_input_grad(g_near, kernel)
        far_sum = part_far[:2] + move(part_far[2:], swap_core)
        near_sum = part_near[:2] + move(part_near[2:], swap_core)
        act_mine = (near_sum + move(far_sum, swap_chip)).astype(jnp.bfloat16)
        act_back = move(act_mine, to_home)

        w_total = conv_kernel_grad(xs[0], gs[0])
        for x_r, g_r in zip(xs[1:], gs[1:]):
            w_total = w_total + conv_kernel_grad(x_r, g_r)

        z_rel = jnp.concatenate([z_near, z_far]).reshape(4, 2, 14, 14, -1)
        z_local = jnp.concatenate([lax.dynamic_index_in_dim(z_rel, jnp.bitwise_xor(tp, j), 0, keepdims=False) for j in range(4)])
        z_keep = jnp.where(on_conv, z_local, jnp.zeros_like(z_local))
        w_keep = jnp.where(on_conv, w_total, jnp.zeros_like(w_total))
        return z_keep[None], act_back[None], w_keep[None]

    return jax.shard_map(device_step, mesh=mesh, in_specs=(act_spec, w_spec, vec_spec, vec_spec, chan_spec), out_specs=(chan_spec, act_spec, w_spec), check_vma=False)
```

```python
import functools

import jax
import jax.numpy as jnp
from jax import lax
from jax.experimental import pallas as pl
from jax.experimental.pallas import tpu as pltpu
from jax.sharding import PartitionSpec as P

MESH = pl.DeviceIdType.MESH
F32 = jnp.float32
BF16 = jnp.bfloat16

SIDE = 14
LINE = 16
ROWS = SIDE * LINE
IMG = 256
PAIR = 2 * IMG
NDP = 4
GROUPS = ((0, 1), (2, 3), (4, 5), (6, 7), (8, 9), (12, 13), (10, 14), (11, 15))


def widen(dst, n, src, m):
    dst[n] = jnp.zeros(dst.shape[1:], BF16)
    for h in range(SIDE):
        dst[n, pl.ds(h * LINE, SIDE), :] = src[m, h]


def body(x_ref, w_hbm, gamma_ref, beta_ref, dz_ref, z_ref, dx_ref, dw_ref,
         xbuf, wbuf, gbuf, gs, xt, dxp, dxd, dxx, xs, dxin, dzp,
         w_sem, x_recv, y_send, yf_send, ring_send, x0_send, hop_send, near_send, far_send, early_send,
         g_recv, g_send, d_recv, d_send, h_recv, h_send, b_recv, b_send, m_recv, m_send):
    dp = lax.axis_index('dp')
    stage = lax.axis_index('stage')
    tp = lax.axis_index('tp')
    col, core = tp // 2, tp % 2
    up = (dp + 1) % NDP
    down = (dp + NDP - 1) % NDP
    twin = col * 2 + (1 - core)
    across = (1 - col) * 2 + core
    ci = x_ref.shape[-1]
    co = dz_ref.shape[-1]

    w_copy = pltpu.make_async_copy(w_hbm, wbuf, w_sem)

    @pl.when(stage == 1)
    def _():
        w_copy.start()

    @pl.when(stage == 0)
    def _():
        for i in range(2):
            widen(xs, i, x_ref, i)

    barrier = pltpu.get_barrier_semaphore()
    for peer in ((dp, 1 - stage, tp), (up, stage, tp), (down, stage, tp), (dp, stage, twin), (dp, stage, across)):
        pl.semaphore_signal(barrier, inc=1, device_id=peer, device_id_type=MESH)
    pl.semaphore_wait(barrier, 5)

    def pair(k, j, i):
        return (k * 2 + j) * 2 + i

    def xrows(k, rel, i):
        return xbuf.at[pl.ds(LINE + (pair(k, rel // 2, i) * 2 + rel % 2) * IMG, ROWS), :]

    def copy(src, dst, send, recv, peer):
        return pltpu.make_async_remote_copy(src_ref=src, dst_ref=dst, send_sem=send, recv_sem=recv, device_id=peer, device_id_type=MESH)

    home = (dp, 0, tp)
    conv = (dp, 1, tp)

    def x_source(k, i):
        return xs.at[i] if k == 0 else xrows(k, 0, i)

    def y_copy(k, i):
        return copy(x_source(k, i), xrows(k, 0, i), y_send.at[k, i], x_recv.at[k, 0, i], conv)

    def ring_copy(k, i):
        return copy(x_source(k - 1, i), xrows(k, 0, i), ring_send.at[k, i], x_recv.at[k, 0, i], (up, 0, tp))

    def x0_copy(i):
        return copy(xrows(2, 0, i), xrows(2, 2, i), x0_send.at[i], x_recv.at[2, 2, i], (dp, 0, across))

    def yf_copy(i):
        return copy(xrows(2, 2, i), xrows(2, 2, i), yf_send.at[i], x_recv.at[2, 2, i], conv)

    def hop_copy(k, i):
        return copy(xrows(k, 0, i), xrows(k, 2, i), hop_send.at[k, i], x_recv.at[k, 2, i], (dp, 1, across))

    def early_copy():
        return copy(xrows(0, 0, 0), xrows(1, 0, 0), early_send, x_recv.at[1, 0, 0], (up, 1, tp))

    def near_copy(k, i):
        return copy(xrows(k, 0, i), xrows(k, 1, i), near_send.at[k, i], x_recv.at[k, 1, i], (dp, 1, twin))

    def far_copy(k, i):
        return copy(xrows(k, 2, i), xrows(k, 3, i), far_send.at[k, i], x_recv.at[k, 3, i], (dp, 1, twin))

    def g_copy(k, p):
        rows = pl.ds(0, ROWS)
        return copy(gbuf.at[(k - 1) * 4 + p, :, rows, :], gbuf.at[k * 4 + p, :, rows, :], g_send.at[k, p], g_recv.at[k, p], (up, 1, tp))

    def d_copy(p):
        return copy(dxp.at[p, 1, pl.ds(0, ROWS), :], dxd.at[p], d_send.at[p], d_recv.at[p], (dp, 1, twin))

    own = pl.ds(0, ROWS)

    def h_copy():
        return copy(dxp.at[2, 0, own, :], dxx, h_send, h_recv, (dp, 1, across))

    def b_copy():
        return copy(xs.at[0], dxin, b_send, b_recv, home)

    def m_far():
        return copy(dxp.at[3, 0, own, :], dxd.at[0], m_send.at[0], m_recv.at[0], home)

    def m_cross():
        return copy(dxd.at[0], dxd.at[1], m_send.at[1], m_recv.at[1], (dp, 0, across))

    def m_near():
        return copy(dxp.at[1, 0, own, :], dxd.at[2], m_send.at[2], m_recv.at[2], home)

    def narrow(value):
        return value.reshape(SIDE, LINE, value.shape[-1])[:, :SIDE, :]

    @pl.when(stage == 0)
    def _():
        for i in range(2):
            y_copy(0, i).start()
            ring_copy(1, i).start()
        dw_ref[...] = jnp.zeros_like(dw_ref)
        z_ref[...] = jnp.zeros_like(z_ref)
        ring_copy(1, 0).wait_recv()
        ring_copy(2, 0).start()
        ring_copy(1, 1).wait_recv()
        y_copy(1, 1).start()
        ring_copy(2, 1).start()
        for i in range(2):
            ring_copy(2, i).wait_recv()
            y_copy(2, i).start()
            ring_copy(3, i).start()
            x0_copy(i).start()
        for i in range(2):
            ring_copy(3, i).wait_recv()
            y_copy(3, i).start()
        for i in range(2):
            x0_copy(i).wait_recv()
            yf_copy(i).start()
        m_far().wait_recv()
        m_cross().start()
        m_cross().wait_recv()
        m_near().wait_recv()
        dx_ref[1] = narrow((dxd[2] + dxd[1]).astype(BF16))
        b_copy().wait_recv()
        dx_ref[0] = narrow(dxin[...])
        for i in range(2):
            for k in range(4):
                if (k, i) != (1, 0):
                    y_copy(k, i).wait_send()
                if k:
                    ring_copy(k, i).wait_send()
            x0_copy(i).wait_send()
            yf_copy(i).wait_send()
        m_cross().wait_send()

    def near(k, i):
        y_copy(k, i).wait_recv()
        if k != 2:
            hop_copy(k, i).start()
        near_copy(k, i).start()

    def far(k, i):
        hop_copy(k, i).wait_recv()
        far_copy(k, i).start()

    def g_pass(k, p):
        g_copy(k, p).wait_recv()
        if k < 3:
            g_copy(k + 1, p).start()

    def rolled(value, shift):
        return pltpu.roll(value, shift % value.shape[0], axis=0)

    def forward(p):
        base = LINE + p * PAIR
        rows = PAIR - LINE
        total = None
        for dw in (0, 1, -1):
            part = None
            for dh in (-1, 0, 1):
                lhs = xbuf[pl.ds(pl.multiple_of(base + LINE * dh, LINE), rows), :]
                prod = jnp.dot(lhs, wbuf[(dh + 1) * 3 + dw + 1], preferred_element_type=F32)
                part = prod if part is None else part + prod
            part = rolled(part, -dw) if dw else part
            total = part if total is None else total + part
        affine = total * gamma_ref[...] + beta_ref[...]
        j, i = p // 2, p % 2
        for b in range(2):
            image = ((col + j - 2 * col * j) * 2 + (core + b - 2 * core * b)) * 2 + i
            part = affine[b * IMG:b * IMG + ROWS]
            z_ref[image] = narrow(jnp.maximum(part, 0.0).astype(BF16))
            dz = dzp[image].astype(F32)
            gbuf[p, b, pl.ds(0, ROWS), :] = jnp.where(part > 0, dz * gamma_ref[...], 0.0).astype(BF16)
        g_copy(1, p).start()

    def spread_g(p, at):
        g = gbuf[p].reshape(PAIR, co)
        gf = g.astype(F32)
        to = pl.ds(at, PAIR)
        gs[1, to, :] = g
        gs[2, to, :] = rolled(gf, 1).astype(BF16)
        gs[0, to, :] = rolled(gf, -1).astype(BF16)

    def input_grad(p):
        spread_g(p, LINE)

        def step(n, _):
            at = pl.ds(pl.multiple_of(n * 256, 256), 256)
            acc = None
            for dw in range(3):
                for dh in range(3):
                    lhs = gs[dw, pl.ds(LINE - LINE * (dh - 1), PAIR), :]
                    prod = lax.dot_general(lhs, wbuf[dh * 3 + dw, at, :], (((1,), (1,)), ((), ())), preferred_element_type=F32)
                    acc = prod if acc is None else acc + prod
            dxp[p, 0, :, at] = acc[:IMG]
            dxp[p, 1, :, at] = acc[IMG:]
            return 0

        lax.fori_loop(0, ci // 256, step, 0)
        d_copy(p).start()

    def dx_sum(p):
        d_copy(p).wait_recv()
        dxp[p, 0, own, :] += dxd[p]

    def kernel_grad(first, second):
        spread_g(first, LINE)
        spread_g(second, LINE + PAIR)

        def turn(q, _):
            row = jnp.where(q < 2, first * 2 + q, second * 2 + q - 2)
            at = pl.ds(pl.multiple_of(LINE + row * IMG, LINE), IMG)
            to = pl.ds(pl.multiple_of(q * IMG, IMG), IMG)
            for c in range(ci // 256):
                xt[pl.ds(c * 256, 256), to] = xbuf[at, pl.ds(c * 256, 256)].T
            return 0

        lax.fori_loop(0, 4, turn, 0)

        def step(dw, _):
            for dh in range(3):
                rhs = gs[dw, pl.ds(LINE - LINE * (dh - 1), 2 * PAIR), :]
                dw_ref[dh * 3 + dw] += jnp.dot(xt[...], rhs, preferred_element_type=F32)
            return 0

        lax.fori_loop(0, 3, step, 0)

    @pl.when(stage == 1)
    def _():
        xbuf[pl.ds(0, LINE), :] = jnp.zeros((LINE, ci), BF16)

        def clear(n, _):
            xbuf[pl.ds(pl.multiple_of(LINE + n * IMG + ROWS, LINE), IMG - ROWS), :] = jnp.zeros((IMG - ROWS, ci), BF16)
            return 0

        lax.fori_loop(0, 32, clear, 0)

        def clear_g(n, _):
            gbuf[n, :, pl.ds(ROWS, IMG - ROWS), :] = jnp.zeros((2, IMG - ROWS, co), BF16)
            return 0

        lax.fori_loop(0, 16, clear_g, 0)
        for dw in range(3):
            for at in (0, LINE + PAIR, LINE + 2 * PAIR):
                gs[dw, pl.ds(at, LINE), :] = jnp.zeros((LINE, co), BF16)

        def widen_dz(n, _):
            widen(dzp, n, dz_ref, n)
            return 0

        lax.fori_loop(0, 8, widen_dz, 0)
        dw_ref[...] = jnp.zeros_like(dw_ref)
        dx_ref[...] = jnp.zeros_like(dx_ref)
        w_copy.wait()

        near(0, 0)
        early_copy().start()
        near_copy(0, 0).wait_recv()
        forward(0)
        input_grad(0)
        near(0, 1)
        near(1, 0)
        far(0, 0)
        near_copy(0, 1).wait_recv()
        forward(1)
        g_pass(1, 0)
        far_copy(0, 0).wait_recv()
        forward(2)
        input_grad(2)
        far(0, 1)
        near(1, 1)
        far_copy(0, 1).wait_recv()
        forward(3)
        dx_sum(2)
        g_pass(1, 1)
        h_copy().start()
        input_grad(3)
        g_pass(1, 2)
        near(2, 0)
        dx_sum(3)
        far(1, 0)
        m_far().start()
        input_grad(1)
        dx_sum(0)
        g_pass(1, 3)
        g_pass(2, 0)
        dx_sum(1)
        g_pass(2, 1)
        m_near().start()

        def events(step):
            if step == 1:
                near(2, 1)
                far(1, 1)
                g_pass(2, 2)
                g_pass(2, 3)
            if step == 2:
                for i in range(2):
                    near_copy(1, i).wait_recv()
                g_pass(3, 0)
            if step == 3:
                near(3, 0)
                for i in range(2):
                    far_copy(1, i).wait_recv()
                g_pass(3, 1)
            if step == 4:
                near(3, 1)
                for i in range(2):
                    near_copy(2, i).wait_recv()
                g_pass(3, 2)
            if step == 5:
                for i in range(2):
                    near_copy(3, i).wait_recv()
                g_pass(3, 3)
                h_copy().wait_recv()
                xs[0] = (dxp[0, 0, own, :] + dxx[...]).astype(BF16)
                b_copy().start()
            if step >= 6:
                i = step - 6
                far(2, i)
                far(3, i)
                far_copy(2, i).wait_recv()
                far_copy(3, i).wait_recv()

        def run(step, _):
            for s in range(1, 8):
                @pl.when(step == s)
                def _(s=s):
                    events(s)

            first, second = (jnp.int32(v) for v in GROUPS[0])
            for s in range(1, 8):
                first = jnp.where(step == s, GROUPS[s][0], first)
                second = jnp.where(step == s, GROUPS[s][1], second)
            kernel_grad(first, second)
            return 0

        lax.fori_loop(0, 8, run, 0)

        for i in range(2):
            for k in range(4):
                near_copy(k, i).wait_send()
                far_copy(k, i).wait_send()
                if k != 2:
                    hop_copy(k, i).wait_send()
        early_copy().wait_send()
        for p in range(4):
            d_copy(p).wait_send()
            for k in range(1, 4):
                g_copy(k, p).wait_send()
        h_copy().wait_send()
        b_copy().wait_send()
        m_far().wait_send()
        m_near().wait_send()


def solution(mesh):
    act_spec = P('stage', ('dp', 'tp'))
    w_spec = P('stage', None, None, None, 'tp')
    vec_spec = P('stage', 'tp')
    chan_spec = P('stage', 'dp', None, None, 'tp')

    def device_step(act_in, w_conv, gamma_vec, beta_vec, z_grad):
        ci, co = w_conv.shape[3], w_conv.shape[4]
        w = w_conv[0].reshape(9, ci, co)
        vmem = pl.BlockSpec(memory_space=pltpu.VMEM)
        dma = pltpu.SemaphoreType.DMA
        z, dx, dw = pl.pallas_call(
            body,
            out_shape=(
                jax.ShapeDtypeStruct((8, SIDE, SIDE, co), BF16),
                jax.ShapeDtypeStruct((2, SIDE, SIDE, ci), BF16),
                jax.ShapeDtypeStruct((9, ci, co), F32),
            ),
            in_specs=[vmem, pl.BlockSpec(memory_space=pl.ANY), vmem, vmem, vmem],
            out_specs=[vmem, vmem, vmem],
            scratch_shapes=[
                pltpu.VMEM((LINE + 16 * PAIR, ci), BF16),
                pltpu.VMEM((9, ci, co), BF16),
                pltpu.VMEM((16, 2, IMG, co), BF16),
                pltpu.VMEM((3, LINE + 2 * PAIR + LINE, co), BF16),
                pltpu.VMEM((ci, 2 * PAIR), BF16),
                pltpu.VMEM((4, 2, IMG, ci), F32),
                pltpu.VMEM((4, ROWS, ci), F32),
                pltpu.VMEM((ROWS, ci), F32),
                pltpu.VMEM((2, ROWS, ci), BF16),
                pltpu.VMEM((ROWS, ci), BF16),
                pltpu.VMEM((8, ROWS, co), BF16),
                dma, dma((4, 4, 2)), dma((4, 2)), dma((2,)), dma((4, 2)), dma((2,)), dma((4, 2)), dma((4, 2)), dma((4, 2)), dma,
                dma((4, 4)), dma((4, 4)), dma((4,)), dma((4,)), dma, dma, dma, dma, dma((3,)), dma((3,)),
            ],
            compiler_params=pltpu.CompilerParams(collective_id=0, has_side_effects=True, vmem_limit_bytes=67043328),
            name='conv_block',
        )(act_in[0], w, gamma_vec, beta_vec, z_grad[0])
        return z[None], dx[None], dw.reshape(1, 3, 3, ci, co)

    return jax.shard_map(device_step, mesh=mesh, in_specs=(act_spec, w_spec, vec_spec, vec_spec, chan_spec), out_specs=(chan_spec, act_spec, w_spec), check_vma=False)
```

```python
import functools

import jax
import jax.numpy as jnp
from jax import lax
from jax.experimental import pallas as pl
from jax.experimental.pallas import tpu as pltpu
from jax.sharding import PartitionSpec as P

MESH = pl.DeviceIdType.MESH
F32 = jnp.float32
BF16 = jnp.bfloat16

SIDE = 14
LINE = 16
ROWS = SIDE * LINE
IMG = 256
PAIR = 2 * IMG
NDP = 4
M_PARTS = (pl.ds(0, 512), pl.ds(512, 512))
GROUPS = ((0, 1), (2, 3), (4, 5), (6, 7), (8, 9), (12, 13), (10, 14), (11, 15))


def widen(dst, n, src):
    dst[n] = jnp.zeros(dst.shape[1:], BF16)
    for h in range(SIDE):
        dst[n, pl.ds(h * LINE, SIDE), :] = src[h, :, n, :]


def finish(x_hbm, g_hbm, part_hbm, out_hbm, xt, gs, acc, x_sem, g_sem, in_sem, out_sem):
    x_copy = pltpu.make_async_copy(x_hbm, xt, x_sem)
    g_copy = pltpu.make_async_copy(g_hbm, gs, g_sem)

    def load(tap):
        return pltpu.make_async_copy(part_hbm.at[tap], acc.at[tap], in_sem.at[tap])

    def store(tap):
        return pltpu.make_async_copy(acc.at[tap], out_hbm.at[tap], out_sem.at[tap])

    x_copy.start()
    g_copy.start()
    for tap in range(3):
        load(tap).start()
    x_copy.wait()
    g_copy.wait()
    for tap in range(3, 9):
        load(tap).start()

    def step(dh, _):
        for dw in range(3):
            tap = dh * 3 + dw
            rows = pl.ds(pl.multiple_of(2 * LINE - LINE * dh, LINE), 2 * PAIR)
            load(tap).wait()
            for at in M_PARTS:
                acc[tap, at, :] += jnp.dot(xt[at, :], gs[dw, rows, :], preferred_element_type=F32)
            store(tap).start()
        return 0

    lax.fori_loop(0, 3, step, 0)
    for tap in range(9):
        store(tap).wait()


def body(x_ref, w_hbm, gamma_ref, beta_ref, dz_ref, z_ref, dx_ref, dw_hbm, xt, gs,
         xbuf, wbuf, gbuf, dw_ref, dxp, dxd, dxx, xs, dxin, zf,
         w_sem, dw_sem, x_recv, y_send, yf_send, ring_send, x0_send, hop_send, near_send, far_send, early_send,
         g_recv, g_send, d_recv, d_send, h_recv, h_send, b_recv, b_send, m_recv, m_send):
    dp = lax.axis_index('dp')
    stage = lax.axis_index('stage')
    tp = lax.axis_index('tp')
    col, core = tp // 2, tp % 2
    up = (dp + 1) % NDP
    down = (dp + NDP - 1) % NDP
    twin = col * 2 + (1 - core)
    across = (1 - col) * 2 + core
    ci = x_ref.shape[-1]
    co = dz_ref.shape[-1]

    w_copy = pltpu.make_async_copy(w_hbm, wbuf, w_sem)

    def dw_copy(tap):
        return pltpu.make_async_copy(dw_ref.at[tap], dw_hbm.at[tap], dw_sem.at[tap])

    @pl.when(stage == 1)
    def _():
        w_copy.start()

    barrier = pltpu.get_barrier_semaphore()
    for peer in ((dp, 1 - stage, tp), (up, stage, tp), (down, stage, tp), (dp, stage, twin), (dp, stage, across)):
        pl.semaphore_signal(barrier, inc=1, device_id=peer, device_id_type=MESH)

    @pl.when(stage == 0)
    def _():
        for i in range(2):
            widen(xs, i, x_ref)

    pl.semaphore_wait(barrier, 5)

    def pair(k, j, i):
        return (k * 2 + j) * 2 + i

    def xrows(k, rel, i):
        return xbuf.at[pl.ds(LINE + (pair(k, rel // 2, i) * 2 + rel % 2) * IMG, ROWS), :]

    def copy(src, dst, send, recv, peer):
        return pltpu.make_async_remote_copy(src_ref=src, dst_ref=dst, send_sem=send, recv_sem=recv, device_id=peer, device_id_type=MESH)

    home = (dp, 0, tp)
    conv = (dp, 1, tp)

    def x_source(k, i):
        return xs.at[i] if k == 0 else xrows(k, 0, i)

    def y_copy(k, i):
        return copy(x_source(k, i), xrows(k, 0, i), y_send.at[k, i], x_recv.at[k, 0, i], conv)

    def ring_copy(k, i):
        return copy(x_source(k - 1, i), xrows(k, 0, i), ring_send.at[k, i], x_recv.at[k, 0, i], (up, 0, tp))

    def x0_copy(i):
        return copy(xrows(2, 0, i), xrows(2, 2, i), x0_send.at[i], x_recv.at[2, 2, i], (dp, 0, across))

    def yf_copy(i):
        return copy(xrows(2, 2, i), xrows(2, 2, i), yf_send.at[i], x_recv.at[2, 2, i], conv)

    def hop_copy(k, i):
        return copy(xrows(k, 0, i), xrows(k, 2, i), hop_send.at[k, i], x_recv.at[k, 2, i], (dp, 1, across))

    def early_copy():
        return copy(xrows(0, 0, 0), xrows(1, 0, 0), early_send, x_recv.at[1, 0, 0], (up, 1, tp))

    def near_copy(k, i):
        return copy(xrows(k, 0, i), xrows(k, 1, i), near_send.at[k, i], x_recv.at[k, 1, i], (dp, 1, twin))

    def far_copy(k, i):
        return copy(xrows(k, 2, i), xrows(k, 3, i), far_send.at[k, i], x_recv.at[k, 3, i], (dp, 1, twin))

    def g_copy(k, p):
        rows = pl.ds(0, ROWS)
        return copy(gbuf.at[(k - 1) * 4 + p, :, rows, :], gbuf.at[k * 4 + p, :, rows, :], g_send.at[k, p], g_recv.at[k, p], (up, 1, tp))

    def d_copy(p):
        return copy(dxp.at[p, 1, pl.ds(0, ROWS), :], dxd.at[p], d_send.at[p], d_recv.at[p], (dp, 1, twin))

    own = pl.ds(0, ROWS)

    def h_copy():
        return copy(dxp.at[3, 0, own, :], dxx, h_send, h_recv, (dp, 1, across))

    def b_copy():
        return copy(xs.at[0], dxin, b_send, b_recv, home)

    def m_far():
        return copy(dxp.at[2, 0, own, :], dxd.at[0], m_send.at[0], m_recv.at[0], home)

    def m_cross():
        return copy(dxd.at[0], dxd.at[1], m_send.at[1], m_recv.at[1], (dp, 0, across))

    def m_near():
        return copy(dxp.at[0, 0, own, :], dxd.at[2], m_send.at[2], m_recv.at[2], home)

    def put_dx(i, value):
        for h in range(SIDE):
            dx_ref[h, :, i, :] = value[h * LINE:h * LINE + SIDE]

    halves = [(b, pl.ds(b * 128, 128)) for b in range(co // 128)]

    @pl.when(stage == 0)
    def _():
        for i in range(2):
            y_copy(0, i).start()
            ring_copy(1, i).start()
        dw_ref[...] = jnp.zeros_like(dw_ref)
        for tap in range(9):
            dw_copy(tap).start()
        z_ref[...] = jnp.zeros_like(z_ref)
        xt[...] = jnp.zeros_like(xt)
        gs[...] = jnp.zeros_like(gs)
        ring_copy(1, 0).wait_recv()
        ring_copy(2, 0).start()
        ring_copy(1, 1).wait_recv()
        y_copy(1, 1).start()
        ring_copy(2, 1).start()
        for i in range(2):
            ring_copy(2, i).wait_recv()
            y_copy(2, i).start()
            ring_copy(3, i).start()
            x0_copy(i).start()
        for i in range(2):
            ring_copy(3, i).wait_recv()
            y_copy(3, i).start()
        for i in range(2):
            x0_copy(i).wait_recv()
            yf_copy(i).start()
        m_far().wait_recv()
        m_cross().start()
        m_cross().wait_recv()
        m_near().wait_recv()
        put_dx(0, (dxd[2] + dxd[1]).astype(BF16))
        b_copy().wait_recv()
        put_dx(1, dxin[...])
        for i in range(2):
            for k in range(4):
                if (k, i) != (1, 0):
                    y_copy(k, i).wait_send()
                if k:
                    ring_copy(k, i).wait_send()
            x0_copy(i).wait_send()
            yf_copy(i).wait_send()
        m_cross().wait_send()

    def near(k, i):
        y_copy(k, i).wait_recv()
        if k != 2:
            hop_copy(k, i).start()
        near_copy(k, i).start()

    def far(k, i):
        hop_copy(k, i).wait_recv()
        far_copy(k, i).start()

    def g_pass(k, p):
        g_copy(k, p).wait_recv()
        if k < 3:
            g_copy(k + 1, p).start()

    def rolled(value, shift):
        return pltpu.roll(value, shift % value.shape[0], axis=0)

    def forward(p):
        base = LINE + p * PAIR
        rows = PAIR - LINE
        total = None
        for dw in (0, 1, -1):
            part = None
            for dh in (-1, 0, 1):
                lhs = xbuf[pl.ds(pl.multiple_of(base + LINE * dh, LINE), rows), :]
                prod = jnp.dot(lhs, wbuf[(dh + 1) * 3 + dw + 1], preferred_element_type=F32)
                part = prod if part is None else part + prod
            part = rolled(part, -dw) if dw else part
            total = part if total is None else total + part
        affine = total * gamma_ref[...] + beta_ref[...]
        j, i = p // 2, p % 2
        for b in range(2):
            image = ((col + j - 2 * col * j) * 2 + (core + b - 2 * core * b)) * 2 + i
            part = affine[b * IMG:b * IMG + ROWS]
            for c, lanes in halves:
                aff = part[:, c * 128:c * 128 + 128]
                at = pl.ds(image, ROWS, stride=8)
                g = jnp.where(aff > 0, zf[c, at, :] * gamma_ref[:, lanes], 0.0)
                gbuf[p, b, pl.ds(0, ROWS), lanes] = g.astype(BF16)
                zf[c, at, :] = jnp.maximum(aff, 0.0)
        g_copy(1, p).start()

    def spread_g(p, at):
        g = gbuf[p].reshape(PAIR, co)
        gf = g.astype(F32)
        to = pl.ds(at, PAIR)
        gs[1, to, :] = g
        gs[2, to, :] = rolled(gf, 1).astype(BF16)
        gs[0, to, :] = rolled(gf, -1).astype(BF16)

    def input_grad(p):
        spread_g(p, LINE)

        def step(n, _):
            at = pl.ds(pl.multiple_of(n * 256, 256), 256)
            acc = None
            for dw in range(3):
                for dh in range(3):
                    lhs = gs[dw, pl.ds(LINE - LINE * (dh - 1), PAIR), :]
                    prod = lax.dot_general(lhs, wbuf[dh * 3 + dw, at, :], (((1,), (1,)), ((), ())), preferred_element_type=F32)
                    acc = prod if acc is None else acc + prod
            dxp[p, 0, :, at] = acc[:IMG]
            dxp[p, 1, :, at] = acc[IMG:]
            return 0

        lax.fori_loop(0, ci // 256, step, 0)
        d_copy(p).start()

    def dx_sum(p):
        d_copy(p).wait_recv()
        dxp[p, 0, own, :] += dxd[p]

    def prepare(first, second):
        spread_g(first, LINE)
        spread_g(second, LINE + PAIR)

        def turn(q, _):
            row = jnp.where(q < 2, first * 2 + q, second * 2 + q - 2)
            at = pl.ds(pl.multiple_of(LINE + row * IMG, LINE), IMG)
            to = pl.ds(pl.multiple_of(q * IMG, IMG), IMG)
            for c in range(ci // 256):
                xt[pl.ds(c * 256, 256), to] = xbuf[at, pl.ds(c * 256, 256)].T
            return 0

        lax.fori_loop(0, 4, turn, 0)

    def kernel_grad(first, second, last):
        prepare(first, second)

        def step(dw, _):
            for dh in range(3):
                rhs = gs[dw, pl.ds(LINE - LINE * (dh - 1), 2 * PAIR), :]
                for at in M_PARTS:
                    dw_ref[dh * 3 + dw, at, :] += jnp.dot(xt[at, :], rhs, preferred_element_type=F32)

            @pl.when(last)
            def _():
                for dh in range(3):
                    dw_copy(dh * 3 + dw).start()

            return 0

        lax.fori_loop(0, 3, step, 0)

    @pl.when(stage == 1)
    def _():
        xbuf[pl.ds(0, LINE), :] = jnp.zeros((LINE, ci), BF16)

        def clear(n, _):
            xbuf[pl.ds(pl.multiple_of(LINE + n * IMG + ROWS, LINE), IMG - ROWS), :] = jnp.zeros((IMG - ROWS, ci), BF16)
            return 0

        lax.fori_loop(0, 32, clear, 0)

        def clear_g(n, _):
            gbuf[n, :, pl.ds(ROWS, IMG - ROWS), :] = jnp.zeros((2, IMG - ROWS, co), BF16)
            return 0

        lax.fori_loop(0, 16, clear_g, 0)
        for dw in range(3):
            for at in (0, LINE + PAIR, LINE + 2 * PAIR):
                gs[dw, pl.ds(at, LINE), :] = jnp.zeros((LINE, co), BF16)

        for h in range(SIDE):
            for c, lanes in halves:
                zf[c, pl.ds(h * 128, SIDE * 8), :] = dz_ref[h, :, :, lanes].astype(F32).reshape(SIDE * 8, 128)
                zf[c, pl.ds(h * 128 + SIDE * 8, 16), :] = jnp.zeros((16, 128), F32)
        dw_ref[...] = jnp.zeros_like(dw_ref)
        dx_ref[...] = jnp.zeros_like(dx_ref)
        w_copy.wait()

        near(0, 0)
        early_copy().start()
        near_copy(0, 0).wait_recv()
        forward(0)
        input_grad(0)
        near(0, 1)
        far(0, 0)
        near(1, 0)
        dx_sum(0)
        near_copy(0, 1).wait_recv()
        m_near().start()
        forward(1)
        far_copy(0, 0).wait_recv()
        forward(2)
        input_grad(2)
        g_pass(1, 0)
        far(0, 1)
        near(1, 1)
        dx_sum(2)
        g_pass(1, 1)
        m_far().start()
        input_grad(1)
        far_copy(0, 1).wait_recv()
        forward(3)
        g_pass(1, 2)
        input_grad(3)
        near(2, 0)
        far(1, 0)
        dx_sum(1)
        dx_sum(3)
        g_pass(2, 0)
        h_copy().start()
        g_pass(2, 1)

        for h in range(SIDE):
            for c, lanes in halves:
                z_ref[h, :, :, lanes] = zf[c, pl.ds(h * 128, SIDE * 8), :].reshape(SIDE, 8, 128).astype(BF16)

        def events(step):
            if step == 1:
                near(2, 1)
                far(1, 1)
                g_pass(1, 3)
            if step == 2:
                g_pass(2, 2)
                for i in range(2):
                    near_copy(1, i).wait_recv()
            if step == 3:
                near(3, 0)
                for i in range(2):
                    far_copy(1, i).wait_recv()
                g_pass(3, 0)
            if step == 4:
                near(3, 1)
                for i in range(2):
                    near_copy(2, i).wait_recv()
                g_pass(2, 3)
                g_pass(3, 1)
            if step == 5:
                for i in range(2):
                    near_copy(3, i).wait_recv()
                g_pass(3, 2)
                h_copy().wait_recv()
                xs[0] = (dxp[1, 0, own, :] + dxx[...]).astype(BF16)
                b_copy().start()
            if step == 6:
                last_far(0)

        def last_far(i):
            far(2, i)
            far(3, i)
            far_copy(2, i).wait_recv()
            far_copy(3, i).wait_recv()

        def run(step, _):
            for s in range(1, 7):
                @pl.when(step == s)
                def _(s=s):
                    events(s)

            first, second = (jnp.int32(v) for v in GROUPS[0])
            for s in range(1, 7):
                first = jnp.where(step == s, GROUPS[s][0], first)
                second = jnp.where(step == s, GROUPS[s][1], second)
            kernel_grad(first, second, step == 6)
            return 0

        lax.fori_loop(0, 7, run, 0)
        last_far(1)
        g_pass(3, 3)
        prepare(*GROUPS[7])

        for i in range(2):
            for k in range(4):
                near_copy(k, i).wait_send()
                far_copy(k, i).wait_send()
                if k != 2:
                    hop_copy(k, i).wait_send()
        early_copy().wait_send()
        for p in range(4):
            d_copy(p).wait_send()
            for k in range(1, 4):
                g_copy(k, p).wait_send()
        h_copy().wait_send()
        b_copy().wait_send()
        m_far().wait_send()
        m_near().wait_send()

    for tap in range(9):
        dw_copy(tap).wait()


def solution(mesh):
    act_spec = P('stage', ('dp', 'tp'))
    w_spec = P('stage', None, None, None, 'tp')
    vec_spec = P('stage', 'tp')
    chan_spec = P('stage', 'dp', None, None, 'tp')

    def device_step(act_in, w_conv, gamma_vec, beta_vec, z_grad):
        ci, co = w_conv.shape[3], w_conv.shape[4]
        w = w_conv[0].reshape(9, ci, co)
        vmem = pl.BlockSpec(memory_space=pltpu.VMEM)
        dma = pltpu.SemaphoreType.DMA
        z, dx, dw, xt, gs = pl.pallas_call(
            body,
            out_shape=(
                jax.ShapeDtypeStruct((SIDE, SIDE, 8, co), BF16),
                jax.ShapeDtypeStruct((SIDE, SIDE, 2, ci), BF16),
                jax.ShapeDtypeStruct((9, ci, co), F32),
                jax.ShapeDtypeStruct((ci, 2 * PAIR), BF16),
                jax.ShapeDtypeStruct((3, LINE + 2 * PAIR + LINE, co), BF16),
            ),
            in_specs=[vmem, pl.BlockSpec(memory_space=pl.ANY), vmem, vmem, vmem],
            out_specs=[vmem, vmem, pl.BlockSpec(memory_space=pl.ANY), vmem, vmem],
            scratch_shapes=[
                pltpu.VMEM((LINE + 16 * PAIR, ci), BF16),
                pltpu.VMEM((9, ci, co), BF16),
                pltpu.VMEM((16, 2, IMG, co), BF16),
                pltpu.VMEM((9, ci, co), F32),
                pltpu.VMEM((4, 2, IMG, ci), F32),
                pltpu.VMEM((4, ROWS, ci), F32),
                pltpu.VMEM((ROWS, ci), F32),
                pltpu.VMEM((2, ROWS, ci), BF16),
                pltpu.VMEM((ROWS, ci), BF16),
                pltpu.VMEM((co // 128, SIDE * 128, 128), F32),
                dma, dma((9,)), dma((4, 4, 2)), dma((4, 2)), dma((2,)), dma((4, 2)), dma((2,)), dma((4, 2)), dma((4, 2)), dma((4, 2)), dma,
                dma((4, 4)), dma((4, 4)), dma((4,)), dma((4,)), dma, dma, dma, dma, dma((3,)), dma((3,)),
            ],
            compiler_params=pltpu.CompilerParams(collective_id=0, has_side_effects=True, vmem_limit_bytes=67043328),
            name='conv_block',
        )(jnp.transpose(act_in[0], (1, 2, 0, 3)), w, gamma_vec, beta_vec, jnp.transpose(z_grad[0], (1, 2, 0, 3)))
        hbm = pl.BlockSpec(memory_space=pl.ANY)
        dw = pl.pallas_call(
            finish,
            out_shape=jax.ShapeDtypeStruct((9, ci, co), F32),
            in_specs=[hbm, hbm, hbm],
            out_specs=hbm,
            scratch_shapes=[
                pltpu.VMEM(xt.shape, BF16),
                pltpu.VMEM(gs.shape, BF16),
                pltpu.VMEM((9, ci, co), F32),
                dma, dma, dma((9,)), dma((9,)),
            ],
            name='finish',
        )(xt, gs, dw)
        z = jnp.transpose(z, (2, 0, 1, 3))
        dx = jnp.transpose(dx, (2, 0, 1, 3))
        return z[None], dx[None], dw.reshape(1, 3, 3, ci, co)

    return jax.shard_map(device_step, mesh=mesh, in_specs=(act_spec, w_spec, vec_spec, vec_spec, chan_spec), out_specs=(chan_spec, act_spec, w_spec), check_vma=False)
```

```python
import functools

import jax
import jax.numpy as jnp
from jax import lax
from jax.experimental import pallas as pl
from jax.experimental.pallas import tpu as pltpu
from jax.sharding import PartitionSpec as P

MESH = pl.DeviceIdType.MESH
F32 = jnp.float32
BF16 = jnp.bfloat16

SIDE = 14
LINE = 16
ROWS = SIDE * LINE
IMG = 256
PAIR = 2 * IMG
NDP = 4
M_PARTS = (pl.ds(0, 512), pl.ds(512, 512))
GROUPS = ((2, 3), (4, 5), (6, 7), (8, 9), (12, 13), (10, 14), (11, 15))


def widen(dst, n, src):
    dst[n] = jnp.zeros(dst.shape[1:], BF16)
    for h in range(SIDE):
        dst[n, pl.ds(h * LINE, SIDE), :] = src[h, :, n, :]


def finish(x_hbm, g_hbm, part_hbm, out_hbm, xt, gs, acc, x_sem, g_sem, in_sem, out_sem):
    x_copy = pltpu.make_async_copy(x_hbm, xt, x_sem)
    g_copy = pltpu.make_async_copy(g_hbm, gs, g_sem)

    def load(tap):
        return pltpu.make_async_copy(part_hbm.at[tap], acc.at[tap], in_sem.at[tap])

    def store(tap):
        return pltpu.make_async_copy(acc.at[tap], out_hbm.at[tap], out_sem.at[tap])

    x_copy.start()
    g_copy.start()
    for tap in range(3):
        load(tap).start()
    x_copy.wait()
    g_copy.wait()
    for tap in range(3, 9):
        load(tap).start()

    def step(dh, _):
        for dw in range(3):
            tap = dh * 3 + dw
            rows = pl.ds(pl.multiple_of(2 * LINE - LINE * dh, LINE), 2 * PAIR)
            load(tap).wait()
            for at in M_PARTS:
                acc[tap, at, :] += jnp.dot(xt[at, :], gs[dw, rows, :], preferred_element_type=F32)
            store(tap).start()
        return 0

    lax.fori_loop(0, 3, step, 0)
    for tap in range(9):
        store(tap).wait()


def body(x_ref, w_hbm, gamma_ref, beta_ref, dz_ref, z_ref, dx_ref, dw_hbm, xt, gs,
         xbuf, wbuf, gbuf, dw_ref, dxp, dxd, dxx, xs, dxin, zf,
         w_sem, dw_sem, x_recv, y_send, yf_send, ring_send, x0_send, hop_send, near_send, far_send, early_send,
         g_recv, g_send, d_recv, d_send, h_recv, h_send, b_recv, b_send, m_recv, m_send):
    dp = lax.axis_index('dp')
    stage = lax.axis_index('stage')
    tp = lax.axis_index('tp')
    col, core = tp // 2, tp % 2
    up = (dp + 1) % NDP
    down = (dp + NDP - 1) % NDP
    twin = col * 2 + (1 - core)
    across = (1 - col) * 2 + core
    ci = x_ref.shape[-1]
    co = dz_ref.shape[-1]

    w_copy = pltpu.make_async_copy(w_hbm, wbuf, w_sem)

    def dw_copy(tap):
        return pltpu.make_async_copy(dw_ref.at[tap], dw_hbm.at[tap], dw_sem.at[tap])

    @pl.when(stage == 1)
    def _():
        w_copy.start()

    barrier = pltpu.get_barrier_semaphore()
    for peer in ((dp, 1 - stage, tp), (up, stage, tp), (down, stage, tp), (dp, stage, twin), (dp, stage, across)):
        pl.semaphore_signal(barrier, inc=1, device_id=peer, device_id_type=MESH)

    @pl.when(stage == 0)
    def _():
        for i in range(2):
            widen(xs, i, x_ref)

    pl.semaphore_wait(barrier, 5)

    def pair(k, j, i):
        return (k * 2 + j) * 2 + i

    def xrows(k, rel, i):
        return xbuf.at[pl.ds(LINE + (pair(k, rel // 2, i) * 2 + rel % 2) * IMG, ROWS), :]

    def copy(src, dst, send, recv, peer):
        return pltpu.make_async_remote_copy(src_ref=src, dst_ref=dst, send_sem=send, recv_sem=recv, device_id=peer, device_id_type=MESH)

    home = (dp, 0, tp)
    conv = (dp, 1, tp)

    def x_source(k, i):
        return xs.at[i] if k == 0 else xrows(k, 0, i)

    def y_copy(k, i):
        return copy(x_source(k, i), xrows(k, 0, i), y_send.at[k, i], x_recv.at[k, 0, i], conv)

    def ring_copy(k, i):
        return copy(x_source(k - 1, i), xrows(k, 0, i), ring_send.at[k, i], x_recv.at[k, 0, i], (up, 0, tp))

    def x0_copy(i):
        return copy(xrows(2, 0, i), xrows(2, 2, i), x0_send.at[i], x_recv.at[2, 2, i], (dp, 0, across))

    def yf_copy(i):
        return copy(xrows(2, 2, i), xrows(2, 2, i), yf_send.at[i], x_recv.at[2, 2, i], conv)

    def hop_copy(k, i):
        return copy(xrows(k, 0, i), xrows(k, 2, i), hop_send.at[k, i], x_recv.at[k, 2, i], (dp, 1, across))

    def early_copy():
        return copy(xrows(0, 0, 0), xrows(1, 0, 0), early_send, x_recv.at[1, 0, 0], (up, 1, tp))

    def near_copy(k, i):
        return copy(xrows(k, 0, i), xrows(k, 1, i), near_send.at[k, i], x_recv.at[k, 1, i], (dp, 1, twin))

    def far_copy(k, i):
        return copy(xrows(k, 2, i), xrows(k, 3, i), far_send.at[k, i], x_recv.at[k, 3, i], (dp, 1, twin))

    def g_copy(k, p):
        rows = pl.ds(0, ROWS)
        return copy(gbuf.at[(k - 1) * 4 + p, :, rows, :], gbuf.at[k * 4 + p, :, rows, :], g_send.at[k, p], g_recv.at[k, p], (up, 1, tp))

    def d_copy(p):
        return copy(dxp.at[p, 1, pl.ds(0, ROWS), :], dxd.at[p], d_send.at[p], d_recv.at[p], (dp, 1, twin))

    own = pl.ds(0, ROWS)

    def h_copy():
        return copy(dxp.at[3, 0, own, :], dxx, h_send, h_recv, (dp, 1, across))

    def b_copy():
        return copy(xs.at[0], dxin, b_send, b_recv, home)

    def m_far():
        return copy(dxp.at[2, 0, own, :], dxd.at[0], m_send.at[0], m_recv.at[0], home)

    def m_cross():
        return copy(dxd.at[0], dxd.at[1], m_send.at[1], m_recv.at[1], (dp, 0, across))

    def m_near():
        return copy(dxp.at[0, 0, own, :], dxd.at[2], m_send.at[2], m_recv.at[2], home)

    def put_dx(i, value):
        for h in range(SIDE):
            dx_ref[h, :, i, :] = value[h * LINE:h * LINE + SIDE]

    halves = [(b, pl.ds(b * 128, 128)) for b in range(co // 128)]

    @pl.when(stage == 0)
    def _():
        for i in range(2):
            y_copy(0, i).start()
            ring_copy(1, i).start()
        dw_ref[...] = jnp.zeros_like(dw_ref)
        for tap in range(9):
            dw_copy(tap).start()
        z_ref[...] = jnp.zeros_like(z_ref)
        xt[...] = jnp.zeros_like(xt)
        gs[...] = jnp.zeros_like(gs)
        ring_copy(1, 0).wait_recv()
        ring_copy(2, 0).start()
        ring_copy(1, 1).wait_recv()
        y_copy(1, 1).start()
        ring_copy(2, 1).start()
        for i in range(2):
            ring_copy(2, i).wait_recv()
            y_copy(2, i).start()
            ring_copy(3, i).start()
            x0_copy(i).start()
        for i in range(2):
            ring_copy(3, i).wait_recv()
            y_copy(3, i).start()
        for i in range(2):
            x0_copy(i).wait_recv()
            yf_copy(i).start()
        m_far().wait_recv()
        m_cross().start()
        m_cross().wait_recv()
        m_near().wait_recv()
        put_dx(0, (dxd[2] + dxd[1]).astype(BF16))
        b_copy().wait_recv()
        put_dx(1, dxin[...])
        for i in range(2):
            for k in range(4):
                if (k, i) != (1, 0):
                    y_copy(k, i).wait_send()
                if k:
                    ring_copy(k, i).wait_send()
            x0_copy(i).wait_send()
            yf_copy(i).wait_send()
        m_cross().wait_send()

    def near(k, i):
        y_copy(k, i).wait_recv()
        if k != 2:
            hop_copy(k, i).start()
        near_copy(k, i).start()

    def far(k, i):
        hop_copy(k, i).wait_recv()
        far_copy(k, i).start()

    def g_pass(k, p):
        g_copy(k, p).wait_recv()
        if k < 3:
            g_copy(k + 1, p).start()

    def rolled(value, shift):
        return pltpu.roll(value, shift % value.shape[0], axis=0)

    def forward(p):
        base = LINE + p * PAIR
        rows = PAIR - LINE
        total = None
        for dw in (0, 1, -1):
            part = None
            for dh in (-1, 0, 1):
                lhs = xbuf[pl.ds(pl.multiple_of(base + LINE * dh, LINE), rows), :]
                prod = jnp.dot(lhs, wbuf[(dh + 1) * 3 + dw + 1], preferred_element_type=F32)
                part = prod if part is None else part + prod
            part = rolled(part, -dw) if dw else part
            total = part if total is None else total + part
        affine = total * gamma_ref[...] + beta_ref[...]
        j, i = p // 2, p % 2
        for b in range(2):
            image = ((col + j - 2 * col * j) * 2 + (core + b - 2 * core * b)) * 2 + i
            part = affine[b * IMG:b * IMG + ROWS]
            for c, lanes in halves:
                aff = part[:, c * 128:c * 128 + 128]
                at = pl.ds(image, ROWS, stride=8)
                g = jnp.where(aff > 0, zf[c, at, :] * gamma_ref[:, lanes], 0.0)
                gbuf[p, b, pl.ds(0, ROWS), lanes] = g.astype(BF16)
                zf[c, at, :] = jnp.maximum(aff, 0.0)
        g_copy(1, p).start()

    def spread_g(p, at):
        g = gbuf[p].reshape(PAIR, co)
        gf = g.astype(F32)
        to = pl.ds(at, PAIR)
        gs[1, to, :] = g
        gs[2, to, :] = rolled(gf, 1).astype(BF16)
        gs[0, to, :] = rolled(gf, -1).astype(BF16)

    def input_grad(p):
        spread_g(p, LINE)

        def step(n, _):
            at = pl.ds(pl.multiple_of(n * 256, 256), 256)
            acc = None
            for dw in range(3):
                for dh in range(3):
                    lhs = gs[dw, pl.ds(LINE - LINE * (dh - 1), PAIR), :]
                    prod = lax.dot_general(lhs, wbuf[dh * 3 + dw, at, :], (((1,), (1,)), ((), ())), preferred_element_type=F32)
                    acc = prod if acc is None else acc + prod
            dxp[p, 0, :, at] = acc[:IMG]
            dxp[p, 1, :, at] = acc[IMG:]
            return 0

        lax.fori_loop(0, ci // 256, step, 0)
        d_copy(p).start()

    def dx_sum(p):
        d_copy(p).wait_recv()
        dxp[p, 0, own, :] += dxd[p]

    def prepare(first, second):
        spread_g(first, LINE)
        spread_g(second, LINE + PAIR)

        turn_in(0, 4, first, second)

    def turn_in(begin, end, first, second):
        def turn(q, _):
            row = jnp.where(q < 2, first * 2 + q, second * 2 + q - 2)
            at = pl.ds(pl.multiple_of(LINE + row * IMG, LINE), IMG)
            to = pl.ds(pl.multiple_of(q * IMG, IMG), IMG)
            for c in range(ci // 256):
                xt[pl.ds(c * 256, 256), to] = xbuf[at, pl.ds(c * 256, 256)].T
            return 0

        lax.fori_loop(begin, end, turn, 0)

    def kernel_grad(first, second, last):
        prepare(first, second)

        def step(dw, _):
            for dh in range(3):
                rhs = gs[dw, pl.ds(LINE - LINE * (dh - 1), 2 * PAIR), :]
                for at in M_PARTS:
                    dw_ref[dh * 3 + dw, at, :] += jnp.dot(xt[at, :], rhs, preferred_element_type=F32)

            @pl.when(last)
            def _():
                for dh in range(3):
                    dw_copy(dh * 3 + dw).start()

            return 0

        lax.fori_loop(0, 3, step, 0)

    @pl.when(stage == 1)
    def _():
        xbuf[pl.ds(0, LINE), :] = jnp.zeros((LINE, ci), BF16)

        def clear(n, _):
            xbuf[pl.ds(pl.multiple_of(LINE + n * IMG + ROWS, LINE), IMG - ROWS), :] = jnp.zeros((IMG - ROWS, ci), BF16)
            return 0

        lax.fori_loop(0, 32, clear, 0)

        def clear_g(n, _):
            gbuf[n, :, pl.ds(ROWS, IMG - ROWS), :] = jnp.zeros((2, IMG - ROWS, co), BF16)
            return 0

        lax.fori_loop(0, 16, clear_g, 0)
        for dw in range(3):
            for at in (0, LINE + PAIR, LINE + 2 * PAIR):
                gs[dw, pl.ds(at, LINE), :] = jnp.zeros((LINE, co), BF16)

        for h in range(SIDE):
            for c, lanes in halves:
                zf[c, pl.ds(h * 128, SIDE * 8), :] = dz_ref[h, :, :, lanes].astype(F32).reshape(SIDE * 8, 128)
                zf[c, pl.ds(h * 128 + SIDE * 8, 16), :] = jnp.zeros((16, 128), F32)
        dw_ref[...] = jnp.zeros_like(dw_ref)
        dx_ref[...] = jnp.zeros_like(dx_ref)
        w_copy.wait()

        def early_grad(p):
            turn_in(0, 2, p, p)

            def step(dw, _):
                for dh in range(3):
                    rhs = gs[dw, pl.ds(LINE - LINE * (dh - 1), PAIR), :]
                    for at in M_PARTS:
                        dw_ref[dh * 3 + dw, at, :] += jnp.dot(xt[at, 0:PAIR], rhs, preferred_element_type=F32)
                return 0

            lax.fori_loop(0, 3, step, 0)

        near(0, 0)
        early_copy().start()
        near_copy(0, 0).wait_recv()
        forward(0)
        input_grad(0)
        early_grad(0)
        near(0, 1)
        far(0, 0)
        near(1, 0)
        dx_sum(0)
        near_copy(0, 1).wait_recv()
        m_near().start()
        forward(1)
        far_copy(0, 0).wait_recv()
        forward(2)
        input_grad(2)
        g_pass(1, 0)
        far(0, 1)
        near(1, 1)
        dx_sum(2)
        g_pass(1, 1)
        m_far().start()
        input_grad(1)
        early_grad(1)
        far_copy(0, 1).wait_recv()
        forward(3)
        g_pass(1, 2)
        input_grad(3)
        near(2, 0)
        far(1, 0)
        dx_sum(1)
        dx_sum(3)
        g_pass(2, 0)
        h_copy().start()
        g_pass(2, 1)

        for h in range(SIDE):
            for c, lanes in halves:
                z_ref[h, :, :, lanes] = zf[c, pl.ds(h * 128, SIDE * 8), :].reshape(SIDE, 8, 128).astype(BF16)

        near(2, 1)
        far(1, 1)

        def events(step):
            if step == 1:
                g_pass(1, 3)
                g_pass(2, 2)
                for i in range(2):
                    near_copy(1, i).wait_recv()
            if step == 2:
                near(3, 0)
                for i in range(2):
                    far_copy(1, i).wait_recv()
                g_pass(3, 0)
            if step == 3:
                near(3, 1)
                for i in range(2):
                    near_copy(2, i).wait_recv()
                g_pass(2, 3)
                g_pass(3, 1)
            if step == 4:
                for i in range(2):
                    near_copy(3, i).wait_recv()
                g_pass(3, 2)
                h_copy().wait_recv()
                xs[0] = (dxp[1, 0, own, :] + dxx[...]).astype(BF16)
                b_copy().start()
            if step == 5:
                last_far(0)

        def last_far(i):
            far(2, i)
            far(3, i)
            far_copy(2, i).wait_recv()
            far_copy(3, i).wait_recv()

        def run(step, _):
            for s in range(1, 6):
                @pl.when(step == s)
                def _(s=s):
                    events(s)

            first, second = (jnp.int32(v) for v in GROUPS[0])
            for s in range(1, 6):
                first = jnp.where(step == s, GROUPS[s][0], first)
                second = jnp.where(step == s, GROUPS[s][1], second)
            kernel_grad(first, second, step == 5)
            return 0

        lax.fori_loop(0, 6, run, 0)
        last_far(1)
        g_pass(3, 3)
        prepare(*GROUPS[6])

        for i in range(2):
            for k in range(4):
                near_copy(k, i).wait_send()
                far_copy(k, i).wait_send()
                if k != 2:
                    hop_copy(k, i).wait_send()
        early_copy().wait_send()
        for p in range(4):
            d_copy(p).wait_send()
            for k in range(1, 4):
                g_copy(k, p).wait_send()
        h_copy().wait_send()
        b_copy().wait_send()
        m_far().wait_send()
        m_near().wait_send()

    for tap in range(9):
        dw_copy(tap).wait()


def solution(mesh):
    act_spec = P('stage', ('dp', 'tp'))
    w_spec = P('stage', None, None, None, 'tp')
    vec_spec = P('stage', 'tp')
    chan_spec = P('stage', 'dp', None, None, 'tp')

    def device_step(act_in, w_conv, gamma_vec, beta_vec, z_grad):
        ci, co = w_conv.shape[3], w_conv.shape[4]
        w = w_conv[0].reshape(9, ci, co)
        vmem = pl.BlockSpec(memory_space=pltpu.VMEM)
        dma = pltpu.SemaphoreType.DMA
        z, dx, dw, xt, gs = pl.pallas_call(
            body,
            out_shape=(
                jax.ShapeDtypeStruct((SIDE, SIDE, 8, co), BF16),
                jax.ShapeDtypeStruct((SIDE, SIDE, 2, ci), BF16),
                jax.ShapeDtypeStruct((9, ci, co), F32),
                jax.ShapeDtypeStruct((ci, 2 * PAIR), BF16),
                jax.ShapeDtypeStruct((3, LINE + 2 * PAIR + LINE, co), BF16),
            ),
            in_specs=[vmem, pl.BlockSpec(memory_space=pl.ANY), vmem, vmem, vmem],
            out_specs=[vmem, vmem, pl.BlockSpec(memory_space=pl.ANY), vmem, vmem],
            scratch_shapes=[
                pltpu.VMEM((LINE + 16 * PAIR, ci), BF16),
                pltpu.VMEM((9, ci, co), BF16),
                pltpu.VMEM((16, 2, IMG, co), BF16),
                pltpu.VMEM((9, ci, co), F32),
                pltpu.VMEM((4, 2, IMG, ci), F32),
                pltpu.VMEM((4, ROWS, ci), F32),
                pltpu.VMEM((ROWS, ci), F32),
                pltpu.VMEM((2, ROWS, ci), BF16),
                pltpu.VMEM((ROWS, ci), BF16),
                pltpu.VMEM((co // 128, SIDE * 128, 128), F32),
                dma, dma((9,)), dma((4, 4, 2)), dma((4, 2)), dma((2,)), dma((4, 2)), dma((2,)), dma((4, 2)), dma((4, 2)), dma((4, 2)), dma,
                dma((4, 4)), dma((4, 4)), dma((4,)), dma((4,)), dma, dma, dma, dma, dma((3,)), dma((3,)),
            ],
            compiler_params=pltpu.CompilerParams(collective_id=0, has_side_effects=True, vmem_limit_bytes=67043328),
            name='conv_block',
        )(jnp.transpose(act_in[0], (1, 2, 0, 3)), w, gamma_vec, beta_vec, jnp.transpose(z_grad[0], (1, 2, 0, 3)))
        hbm = pl.BlockSpec(memory_space=pl.ANY)
        dw = pl.pallas_call(
            finish,
            out_shape=jax.ShapeDtypeStruct((9, ci, co), F32),
            in_specs=[hbm, hbm, hbm],
            out_specs=hbm,
            scratch_shapes=[
                pltpu.VMEM(xt.shape, BF16),
                pltpu.VMEM(gs.shape, BF16),
                pltpu.VMEM((9, ci, co), F32),
                dma, dma, dma((9,)), dma((9,)),
            ],
            name='finish',
        )(xt, gs, dw)
        z = jnp.transpose(z, (2, 0, 1, 3))
        dx = jnp.transpose(dx, (2, 0, 1, 3))
        return z[None], dx[None], dw.reshape(1, 3, 3, ci, co)

    return jax.shard_map(device_step, mesh=mesh, in_specs=(act_spec, w_spec, vec_spec, vec_spec, chan_spec), out_specs=(chan_spec, act_spec, w_spec), check_vma=False)
```

```python
import functools

import jax
import jax.numpy as jnp
from jax import lax
from jax.experimental import pallas as pl
from jax.experimental.pallas import tpu as pltpu
from jax.sharding import PartitionSpec as P

MESH = pl.DeviceIdType.MESH
F32 = jnp.float32
BF16 = jnp.bfloat16

SIDE = 14
LINE = 16
ROWS = SIDE * LINE
IMG = 256
PAIR = 2 * IMG
NDP = 4
M_PARTS = (pl.ds(0, 512), pl.ds(512, 512))
GROUPS = ((2, 3), (4, 5), (6, 7), (8, 9), (12, 13), (10, 14), (11, 15))


def widen(dst, n, src):
    dst[n] = jnp.zeros(dst.shape[1:], BF16)
    for h in range(SIDE):
        dst[n, pl.ds(h * LINE, SIDE), :] = src[h, :, n, :]


def finish(x_hbm, g_hbm, part_hbm, out_hbm, xt, gs, acc, x_sem, g_sem, in_sem, out_sem):
    x_copy = pltpu.make_async_copy(x_hbm, xt, x_sem)
    g_copy = pltpu.make_async_copy(g_hbm, gs, g_sem)

    def load(tap):
        return pltpu.make_async_copy(part_hbm.at[tap], acc.at[tap], in_sem.at[tap])

    def store(tap):
        return pltpu.make_async_copy(acc.at[tap], out_hbm.at[tap], out_sem.at[tap])

    x_copy.start()
    g_copy.start()
    for tap in range(3):
        load(tap).start()
    x_copy.wait()
    g_copy.wait()
    for tap in range(3, 9):
        load(tap).start()

    def step(dh, _):
        for dw in range(3):
            tap = dh * 3 + dw
            rows = pl.ds(pl.multiple_of(2 * LINE - LINE * dh, LINE), 2 * PAIR)
            load(tap).wait()
            for at in M_PARTS:
                acc[tap, at, :] += jnp.dot(xt[at, :], gs[dw, rows, :], preferred_element_type=F32)
            store(tap).start()
        return 0

    lax.fori_loop(0, 3, step, 0)
    for tap in range(9):
        store(tap).wait()


def body(x_ref, w_hbm, gamma_ref, beta_ref, dz_ref, z_ref, dx_ref, dw_hbm, xt, gs,
         xbuf, wbuf, gbuf, dw_ref, dxp, dxd, dxx, xs, dxin, zf,
         w_sem, dw_sem, x_recv, y_send, yf_send, ring_send, x0_send, hop_send, near_send, far_send, early_send,
         g_recv, g_send, d_recv, d_send, h_recv, h_send, b_recv, b_send, m_recv, m_send):
    dp = lax.axis_index('dp')
    stage = lax.axis_index('stage')
    tp = lax.axis_index('tp')
    col, core = tp // 2, tp % 2
    up = (dp + 1) % NDP
    down = (dp + NDP - 1) % NDP
    twin = col * 2 + (1 - core)
    across = (1 - col) * 2 + core
    ci = x_ref.shape[-1]
    co = dz_ref.shape[-1]

    w_copy = pltpu.make_async_copy(w_hbm, wbuf, w_sem)

    def dw_copy(tap):
        return pltpu.make_async_copy(dw_ref.at[tap], dw_hbm.at[tap], dw_sem.at[tap])

    @pl.when(stage == 1)
    def _():
        w_copy.start()

    barrier = pltpu.get_barrier_semaphore()
    for peer in ((dp, 1 - stage, tp), (up, stage, tp), (down, stage, tp), (dp, stage, twin), (dp, stage, across)):
        pl.semaphore_signal(barrier, inc=1, device_id=peer, device_id_type=MESH)

    @pl.when(stage == 0)
    def _():
        for i in range(2):
            widen(xs, i, x_ref)

    pl.semaphore_wait(barrier, 5)

    def pair(k, j, i):
        return (k * 2 + j) * 2 + i

    def xrows(k, rel, i):
        return xbuf.at[pl.ds(LINE + (pair(k, rel // 2, i) * 2 + rel % 2) * IMG, ROWS), :]

    def copy(src, dst, send, recv, peer):
        return pltpu.make_async_remote_copy(src_ref=src, dst_ref=dst, send_sem=send, recv_sem=recv, device_id=peer, device_id_type=MESH)

    home = (dp, 0, tp)
    conv = (dp, 1, tp)

    def x_source(k, i):
        return xs.at[i] if k == 0 else xrows(k, 0, i)

    def y_copy(k, i):
        return copy(x_source(k, i), xrows(k, 0, i), y_send.at[k, i], x_recv.at[k, 0, i], conv)

    def ring_copy(k, i):
        return copy(x_source(k - 1, i), xrows(k, 0, i), ring_send.at[k, i], x_recv.at[k, 0, i], (up, 0, tp))

    def x0_copy(i):
        return copy(xrows(2, 0, i), xrows(2, 2, i), x0_send.at[i], x_recv.at[2, 2, i], (dp, 0, across))

    def yf_copy(i):
        return copy(xrows(2, 2, i), xrows(2, 2, i), yf_send.at[i], x_recv.at[2, 2, i], conv)

    def hop_copy(k, i):
        return copy(xrows(k, 0, i), xrows(k, 2, i), hop_send.at[k, i], x_recv.at[k, 2, i], (dp, 1, across))

    def early_copy():
        return copy(xrows(0, 0, 0), xrows(1, 0, 0), early_send, x_recv.at[1, 0, 0], (up, 1, tp))

    def near_copy(k, i):
        return copy(xrows(k, 0, i), xrows(k, 1, i), near_send.at[k, i], x_recv.at[k, 1, i], (dp, 1, twin))

    def far_copy(k, i):
        return copy(xrows(k, 2, i), xrows(k, 3, i), far_send.at[k, i], x_recv.at[k, 3, i], (dp, 1, twin))

    def g_copy(k, p):
        rows = pl.ds(0, ROWS)
        return copy(gbuf.at[(k - 1) * 4 + p, :, rows, :], gbuf.at[k * 4 + p, :, rows, :], g_send.at[k, p], g_recv.at[k, p], (up, 1, tp))

    def d_copy(p):
        return copy(dxp.at[p, 1, pl.ds(0, ROWS), :], dxd.at[p], d_send.at[p], d_recv.at[p], (dp, 1, twin))

    own = pl.ds(0, ROWS)

    def h_copy():
        return copy(dxp.at[3, 0, own, :], dxx, h_send, h_recv, (dp, 1, across))

    def b_copy():
        return copy(xs.at[0], dxin, b_send, b_recv, home)

    def m_far():
        return copy(dxp.at[2, 0, own, :], dxd.at[0], m_send.at[0], m_recv.at[0], home)

    def m_cross():
        return copy(dxd.at[0], dxd.at[1], m_send.at[1], m_recv.at[1], (dp, 0, across))

    def m_near():
        return copy(dxp.at[0, 0, own, :], dxd.at[2], m_send.at[2], m_recv.at[2], home)

    def put_dx(i, value):
        for h in range(SIDE):
            dx_ref[h, :, i, :] = value[h * LINE:h * LINE + SIDE]

    halves = [(b, pl.ds(b * 128, 128)) for b in range(co // 128)]

    @pl.when(stage == 0)
    def _():
        for i in range(2):
            y_copy(0, i).start()
            ring_copy(1, i).start()
        dw_ref[...] = jnp.zeros_like(dw_ref)
        for tap in range(9):
            dw_copy(tap).start()
        z_ref[...] = jnp.zeros_like(z_ref)
        xt[...] = jnp.zeros_like(xt)
        gs[...] = jnp.zeros_like(gs)
        ring_copy(1, 0).wait_recv()
        ring_copy(2, 0).start()
        ring_copy(1, 1).wait_recv()
        y_copy(1, 1).start()
        ring_copy(2, 1).start()
        for i in range(2):
            ring_copy(2, i).wait_recv()
            y_copy(2, i).start()
            ring_copy(3, i).start()
            x0_copy(i).start()
        for i in range(2):
            ring_copy(3, i).wait_recv()
            y_copy(3, i).start()
        for i in range(2):
            x0_copy(i).wait_recv()
            yf_copy(i).start()
        m_far().wait_recv()
        m_cross().start()
        m_cross().wait_recv()
        m_near().wait_recv()
        put_dx(0, (dxd[2] + dxd[1]).astype(BF16))
        b_copy().wait_recv()
        put_dx(1, dxin[...])
        for i in range(2):
            for k in range(4):
                if (k, i) != (1, 0):
                    y_copy(k, i).wait_send()
                if k:
                    ring_copy(k, i).wait_send()
            x0_copy(i).wait_send()
            yf_copy(i).wait_send()
        m_cross().wait_send()

    def near(k, i):
        y_copy(k, i).wait_recv()
        if k != 2:
            hop_copy(k, i).start()
        near_copy(k, i).start()

    def far(k, i):
        hop_copy(k, i).wait_recv()
        far_copy(k, i).start()

    def g_pass(k, p):
        g_copy(k, p).wait_recv()
        if k < 3:
            g_copy(k + 1, p).start()

    def rolled(value, shift):
        return pltpu.roll(value, shift % value.shape[0], axis=0)

    def forward(p):
        base = LINE + p * PAIR
        rows = PAIR - LINE
        total = None
        for dw in (0, 1, -1):
            part = None
            for dh in (-1, 0, 1):
                lhs = xbuf[pl.ds(pl.multiple_of(base + LINE * dh, LINE), rows), :]
                prod = jnp.dot(lhs, wbuf[(dh + 1) * 3 + dw + 1], preferred_element_type=F32)
                part = prod if part is None else part + prod
            part = rolled(part, -dw) if dw else part
            total = part if total is None else total + part
        affine = total * gamma_ref[...] + beta_ref[...]
        j, i = p // 2, p % 2
        for b in range(2):
            image = ((col + j - 2 * col * j) * 2 + (core + b - 2 * core * b)) * 2 + i
            part = affine[b * IMG:b * IMG + ROWS]
            for c, lanes in halves:
                aff = part[:, c * 128:c * 128 + 128]
                at = pl.ds(image, ROWS, stride=8)
                g = jnp.where(aff > 0, zf[c, at, :] * gamma_ref[:, lanes], 0.0)
                gbuf[p, b, pl.ds(0, ROWS), lanes] = g.astype(BF16)
                zf[c, at, :] = jnp.maximum(aff, 0.0)
        g_copy(1, p).start()

    def spread_g(p, at):
        g = gbuf[p].reshape(PAIR, co)
        gf = g.astype(F32)
        to = pl.ds(at, PAIR)
        gs[1, to, :] = g
        gs[2, to, :] = rolled(gf, 1).astype(BF16)
        gs[0, to, :] = rolled(gf, -1).astype(BF16)

    def input_grad(p):
        spread_g(p, LINE)

        def step(n, _):
            at = pl.ds(pl.multiple_of(n * 256, 256), 256)
            acc = None
            for dw in range(3):
                for dh in range(3):
                    lhs = gs[dw, pl.ds(LINE - LINE * (dh - 1), PAIR), :]
                    prod = lax.dot_general(lhs, wbuf[dh * 3 + dw, at, :], (((1,), (1,)), ((), ())), preferred_element_type=F32)
                    acc = prod if acc is None else acc + prod
            dxp[p, 0, :, at] = acc[:IMG]
            dxp[p, 1, :, at] = acc[IMG:]
            return 0

        lax.fori_loop(0, ci // 256, step, 0)
        d_copy(p).start()

    def dx_sum(p):
        d_copy(p).wait_recv()
        dxp[p, 0, own, :] += dxd[p]

    def prepare(first, second):
        spread_g(first, LINE)
        spread_g(second, LINE + PAIR)

        turn_in(0, 4, first, second)

    def turn_in(begin, end, first, second):
        def turn(q, _):
            row = jnp.where(q < 2, first * 2 + q, second * 2 + q - 2)
            at = pl.ds(pl.multiple_of(LINE + row * IMG, LINE), IMG)
            to = pl.ds(pl.multiple_of(q * IMG, IMG), IMG)
            for c in range(ci // 256):
                xt[pl.ds(c * 256, 256), to] = xbuf[at, pl.ds(c * 256, 256)].T
            return 0

        lax.fori_loop(begin, end, turn, 0)

    def kernel_grad(first, second, last):
        prepare(first, second)

        def step(dw, _):
            for dh in range(3):
                rhs = gs[dw, pl.ds(LINE - LINE * (dh - 1), 2 * PAIR), :]
                for at in M_PARTS:
                    dw_ref[dh * 3 + dw, at, :] += jnp.dot(xt[at, :], rhs, preferred_element_type=F32)

            @pl.when(last)
            def _():
                for dh in range(3):
                    dw_copy(dh * 3 + dw).start()

            return 0

        lax.fori_loop(0, 3, step, 0)

    @pl.when(stage == 1)
    def _():
        xbuf[pl.ds(0, LINE), :] = jnp.zeros((LINE, ci), BF16)

        def clear(n, _):
            xbuf[pl.ds(pl.multiple_of(LINE + n * IMG + ROWS, LINE), IMG - ROWS), :] = jnp.zeros((IMG - ROWS, ci), BF16)
            return 0

        lax.fori_loop(0, 32, clear, 0)

        def clear_g(n, _):
            gbuf[n, :, pl.ds(ROWS, IMG - ROWS), :] = jnp.zeros((2, IMG - ROWS, co), BF16)
            return 0

        lax.fori_loop(0, 16, clear_g, 0)
        for dw in range(3):
            for at in (0, LINE + PAIR, LINE + 2 * PAIR):
                gs[dw, pl.ds(at, LINE), :] = jnp.zeros((LINE, co), BF16)

        for h in range(SIDE):
            for c, lanes in halves:
                zf[c, pl.ds(h * 128, SIDE * 8), :] = dz_ref[h, :, :, lanes].astype(F32).reshape(SIDE * 8, 128)
                zf[c, pl.ds(h * 128 + SIDE * 8, 16), :] = jnp.zeros((16, 128), F32)
        dw_ref[...] = jnp.zeros_like(dw_ref)
        dx_ref[...] = jnp.zeros_like(dx_ref)
        w_copy.wait()

        def early_grad(p):
            turn_in(0, 2, p, p)

            def step(dw, _):
                for dh in range(3):
                    rhs = gs[dw, pl.ds(LINE - LINE * (dh - 1), PAIR), :]
                    for at in M_PARTS:
                        dw_ref[dh * 3 + dw, at, :] += jnp.dot(xt[at, 0:PAIR], rhs, preferred_element_type=F32)
                return 0

            lax.fori_loop(0, 3, step, 0)

        near(0, 0)
        early_copy().start()
        near_copy(0, 0).wait_recv()
        forward(0)
        input_grad(0)
        early_grad(0)
        near(0, 1)
        far(0, 0)
        near(1, 0)
        dx_sum(0)
        near_copy(0, 1).wait_recv()
        m_near().start()
        forward(1)
        far_copy(0, 0).wait_recv()
        forward(2)
        input_grad(2)
        g_pass(1, 0)
        far(0, 1)
        near(1, 1)
        dx_sum(2)
        g_pass(1, 1)
        m_far().start()
        input_grad(1)
        early_grad(1)
        far_copy(0, 1).wait_recv()
        forward(3)
        g_pass(1, 2)
        input_grad(3)
        near(2, 0)
        far(1, 0)
        dx_sum(1)
        dx_sum(3)
        g_pass(2, 0)
        h_copy().start()
        g_pass(2, 1)

        for h in range(SIDE):
            for c, lanes in halves:
                z_ref[h, :, :, lanes] = zf[c, pl.ds(h * 128, SIDE * 8), :].reshape(SIDE, 8, 128).astype(BF16)

        near(2, 1)
        far(1, 1)

        def events(step):
            if step == 1:
                g_pass(1, 3)
                g_pass(2, 2)
                for i in range(2):
                    near_copy(1, i).wait_recv()
            if step == 2:
                near(3, 0)
                for i in range(2):
                    far_copy(1, i).wait_recv()
                g_pass(3, 0)
            if step == 3:
                near(3, 1)
                for i in range(2):
                    near_copy(2, i).wait_recv()
            if step == 4:
                for i in range(2):
                    near_copy(3, i).wait_recv()
                g_pass(2, 3)
                g_pass(3, 1)
                h_copy().wait_recv()
                xs[0] = (dxp[1, 0, own, :] + dxx[...]).astype(BF16)
                b_copy().start()
            if step == 5:
                g_pass(3, 2)
                last_far(0)

        def last_far(i):
            far(2, i)
            far(3, i)
            far_copy(2, i).wait_recv()
            far_copy(3, i).wait_recv()

        def run(step, _):
            for s in range(1, 6):
                @pl.when(step == s)
                def _(s=s):
                    events(s)

            first, second = (jnp.int32(v) for v in GROUPS[0])
            for s in range(1, 6):
                first = jnp.where(step == s, GROUPS[s][0], first)
                second = jnp.where(step == s, GROUPS[s][1], second)
            kernel_grad(first, second, step == 5)
            return 0

        lax.fori_loop(0, 6, run, 0)
        last_far(1)
        g_pass(3, 3)
        prepare(*GROUPS[6])

        for i in range(2):
            for k in range(4):
                near_copy(k, i).wait_send()
                far_copy(k, i).wait_send()
                if k != 2:
                    hop_copy(k, i).wait_send()
        early_copy().wait_send()
        for p in range(4):
            d_copy(p).wait_send()
            for k in range(1, 4):
                g_copy(k, p).wait_send()
        h_copy().wait_send()
        b_copy().wait_send()
        m_far().wait_send()
        m_near().wait_send()

    for tap in range(9):
        dw_copy(tap).wait()


def solution(mesh):
    act_spec = P('stage', ('dp', 'tp'))
    w_spec = P('stage', None, None, None, 'tp')
    vec_spec = P('stage', 'tp')
    chan_spec = P('stage', 'dp', None, None, 'tp')

    def device_step(act_in, w_conv, gamma_vec, beta_vec, z_grad):
        ci, co = w_conv.shape[3], w_conv.shape[4]
        w = w_conv[0].reshape(9, ci, co)
        vmem = pl.BlockSpec(memory_space=pltpu.VMEM)
        dma = pltpu.SemaphoreType.DMA
        z, dx, dw, xt, gs = pl.pallas_call(
            body,
            out_shape=(
                jax.ShapeDtypeStruct((SIDE, SIDE, 8, co), BF16),
                jax.ShapeDtypeStruct((SIDE, SIDE, 2, ci), BF16),
                jax.ShapeDtypeStruct((9, ci, co), F32),
                jax.ShapeDtypeStruct((ci, 2 * PAIR), BF16),
                jax.ShapeDtypeStruct((3, LINE + 2 * PAIR + LINE, co), BF16),
            ),
            in_specs=[vmem, pl.BlockSpec(memory_space=pl.ANY), vmem, vmem, vmem],
            out_specs=[vmem, vmem, pl.BlockSpec(memory_space=pl.ANY), vmem, vmem],
            scratch_shapes=[
                pltpu.VMEM((LINE + 16 * PAIR, ci), BF16),
                pltpu.VMEM((9, ci, co), BF16),
                pltpu.VMEM((16, 2, IMG, co), BF16),
                pltpu.VMEM((9, ci, co), F32),
                pltpu.VMEM((4, 2, IMG, ci), F32),
                pltpu.VMEM((4, ROWS, ci), F32),
                pltpu.VMEM((ROWS, ci), F32),
                pltpu.VMEM((2, ROWS, ci), BF16),
                pltpu.VMEM((ROWS, ci), BF16),
                pltpu.VMEM((co // 128, SIDE * 128, 128), F32),
                dma, dma((9,)), dma((4, 4, 2)), dma((4, 2)), dma((2,)), dma((4, 2)), dma((2,)), dma((4, 2)), dma((4, 2)), dma((4, 2)), dma,
                dma((4, 4)), dma((4, 4)), dma((4,)), dma((4,)), dma, dma, dma, dma, dma((3,)), dma((3,)),
            ],
            compiler_params=pltpu.CompilerParams(collective_id=0, has_side_effects=True, vmem_limit_bytes=67043328),
            name='conv_block',
        )(jnp.transpose(act_in[0], (1, 2, 0, 3)), w, gamma_vec, beta_vec, jnp.transpose(z_grad[0], (1, 2, 0, 3)))
        hbm = pl.BlockSpec(memory_space=pl.ANY)
        dw = pl.pallas_call(
            finish,
            out_shape=jax.ShapeDtypeStruct((9, ci, co), F32),
            in_specs=[hbm, hbm, hbm],
            out_specs=hbm,
            scratch_shapes=[
                pltpu.VMEM(xt.shape, BF16),
                pltpu.VMEM(gs.shape, BF16),
                pltpu.VMEM((9, ci, co), F32),
                dma, dma, dma((9,)), dma((9,)),
            ],
            name='finish',
        )(xt, gs, dw)
        z = jnp.transpose(z, (2, 0, 1, 3))
        dx = jnp.transpose(dx, (2, 0, 1, 3))
        return z[None], dx[None], dw.reshape(1, 3, 3, ci, co)

    return jax.shard_map(device_step, mesh=mesh, in_specs=(act_spec, w_spec, vec_spec, vec_spec, chan_spec), out_specs=(chan_spec, act_spec, w_spec), check_vma=False)
```
